32 devices in a mesh: part: 1 (over z), tp: 4 (over y), ep: 8 (over x, core).
Axes of the slice: x: 4, y: 4, z: 1, core: 2. Of those that a mesh axis runs over, the one named last changes fastest.
The devices are a block of a 4x4x8 slice.
Arguments:
- dec_states: bfloat16 [64, 256, 768], P(('part', 'ep'))
- enc_states: bfloat16 [64, 128, 768], P(('part', 'ep'))
- enc_pad: int32 [64, 128], P(('part', 'ep'))
- expert_idx: int32 [64, 256], P(('part', 'ep'))
- self_bias: float32 [12, 256, 256], P('tp')
- gain_self: float32 [768], replicated
- wq_self: bfloat16 [768, 768], P(None, 'tp')
- wk_self: bfloat16 [768, 768], P(None, 'tp')
- wv_self: bfloat16 [768, 768], P(None, 'tp')
- wo_self: bfloat16 [768, 768], P('tp')
- gain_cross: float32 [768], replicated
- wq_cross: bfloat16 [768, 768], P(None, 'tp')
- wk_cross: bfloat16 [768, 768], P(None, 'tp')
- wv_cross: bfloat16 [768, 768], P(None, 'tp')
- wo_cross: bfloat16 [768, 768], P('tp')
- gain_ffn: float32 [768], replicated
- w_router: float32 [768, 32], replicated
- w_in: bfloat16 [32, 768, 3072], P('ep')
- w_out: bfloat16 [32, 3072, 768], P('ep')
Outputs:
- output: bfloat16 [64, 256, 768], P(('part', 'ep'))
All inputs are finite; a program needn't handle non-finite values.
Results may differ from the reference program's by a relative error of at most 0.0193591.
Values are sent between devices in bfloat16 or wider.
A program may use at most 768 MiB of HBM per device.

```python
import math
import jax
import jax.numpy as jnp
from jax import lax

D_MODEL = 768
NUM_HEADS = 12
HEAD_DIM = 64
D_FF = 3072
EXPERTS = 32
GROUPS = 8
BATCH_DEV = 8
DEC_LEN = 256
ENC_LEN = 128

GROUP_BATCH = GROUPS * BATCH_DEV
TOKENS = BATCH_DEV * DEC_LEN
CAPACITY = (5 * TOKENS + 4 * EXPERTS - 1) // (4 * EXPERTS)
HIDDEN = NUM_HEADS * HEAD_DIM
EPSILON = 1e-6
NEG_LARGE = -1e30


def normal_draw(key, shape, scale):
    return jax.random.normal(key, shape, jnp.float32) * scale


def draw_expert_in(key):
    return normal_draw(key, (D_MODEL, D_FF), D_MODEL ** -0.5).astype(jnp.bfloat16)


def draw_expert_out(key):
    return normal_draw(key, (D_FF, D_MODEL), 0.4 * EXPERTS * D_FF ** -0.5).astype(jnp.bfloat16)


def relative_class(length):
    rel_pos = jnp.arange(length)[:, None] - jnp.arange(length)[None, :]
    distance = jnp.maximum(rel_pos, 0)
    far_class = jnp.full(distance.shape, 16, jnp.int32)
    for step_idx in range(1, 16):
        threshold = int(math.ceil(16.0 * 8.0 ** (step_idx / 16.0)))
        far_class = far_class + (distance >= threshold).astype(jnp.int32)
    return jnp.where(distance < 16, distance, far_class)


def draw_layout(key):
    route_keys = jax.random.split(key, 5)
    first_pick = jax.random.randint(route_keys[0], (GROUPS, TOKENS), 0, EXPERTS)
    second_pick = jax.random.randint(route_keys[1], (GROUPS, TOKENS), 0, EXPERTS)
    coin_flip = jax.random.randint(route_keys[2], (GROUPS, TOKENS), 0, 2)
    skewed = jnp.where(coin_flip == 1, first_pick, jnp.minimum(first_pick, second_pick))
    hot_expert = jax.random.randint(route_keys[3], (GROUPS, 1), 0, EXPERTS)
    local_pos = jnp.arange(TOKENS)[None, :]
    expert_idx = jnp.where(local_pos <= CAPACITY, hot_expert, skewed).reshape(GROUP_BATCH, DEC_LEN).astype(jnp.int32)
    pad_min = ENC_LEN // 10
    pad_max = 2 * ENC_LEN // 5
    pad_len = jax.random.randint(route_keys[4], (GROUP_BATCH,), pad_min, pad_max + 1)
    row_ids = jnp.arange(GROUP_BATCH)
    pad_len = jnp.where(row_ids == 0, pad_max, jnp.where(row_ids == 1, pad_min, pad_len))
    enc_pad = (jnp.arange(ENC_LEN)[None, :] >= ENC_LEN - pad_len[:, None]).astype(jnp.int32)
    return enc_pad, expert_idx


def setup_inputs(seed: int = 0, part: int = 0) -> dict:
    base_key = jax.random.key(seed)
    part_keys = jax.random.split(jax.random.fold_in(base_key, part), 3)
    shared_keys = jax.random.split(jax.random.fold_in(base_key, 1000003), 16)
    enc_pad, expert_idx = draw_layout(part_keys[2])
    scale_in = D_MODEL ** -0.5
    scale_query = 2.0 * (D_MODEL * HEAD_DIM) ** -0.5
    scale_out = HIDDEN ** -0.5
    qkv_shape = (D_MODEL, HIDDEN)
    return {
        'dec_states': normal_draw(part_keys[0], (GROUP_BATCH, DEC_LEN, D_MODEL), 0.5).astype(jnp.bfloat16),
        'enc_states': normal_draw(part_keys[1], (GROUP_BATCH, ENC_LEN, D_MODEL), 1.0).astype(jnp.bfloat16),
        'enc_pad': enc_pad,
        'expert_idx': expert_idx,
        'self_bias': normal_draw(shared_keys[0], (NUM_HEADS, 32), 1.0)[:, relative_class(DEC_LEN)],
        'gain_self': jax.random.uniform(shared_keys[1], (D_MODEL,), jnp.float32, 0.25, 1.75),
        'wq_self': normal_draw(shared_keys[2], qkv_shape, scale_query).astype(jnp.bfloat16),
        'wk_self': normal_draw(shared_keys[3], qkv_shape, scale_in).astype(jnp.bfloat16),
        'wv_self': normal_draw(shared_keys[4], qkv_shape, scale_in).astype(jnp.bfloat16),
        'wo_self': normal_draw(shared_keys[5], (HIDDEN, D_MODEL), scale_out).astype(jnp.bfloat16),
        'gain_cross': jax.random.uniform(shared_keys[6], (D_MODEL,), jnp.float32, 0.25, 1.75),
        'wq_cross': normal_draw(shared_keys[7], qkv_shape, scale_query).astype(jnp.bfloat16),
        'wk_cross': normal_draw(shared_keys[8], qkv_shape, scale_in).astype(jnp.bfloat16),
        'wv_cross': normal_draw(shared_keys[9], qkv_shape, scale_in).astype(jnp.bfloat16),
        'wo_cross': normal_draw(shared_keys[10], (HIDDEN, D_MODEL), scale_out).astype(jnp.bfloat16),
        'gain_ffn': jax.random.uniform(shared_keys[11], (D_MODEL,), jnp.float32, 0.25, 1.75),
        'w_router': normal_draw(shared_keys[12], (D_MODEL, EXPERTS), scale_in),
        'w_in': lax.map(draw_expert_in, jax.random.split(shared_keys[13], EXPERTS)),
        'w_out': lax.map(draw_expert_out, jax.random.split(shared_keys[14], EXPERTS)),
    }


def rms_norm(states, gain_vec):
    upcast = states.astype(jnp.float32)
    mean_sq = jnp.mean(upcast * upcast, axis=-1, keepdims=True)
    return (upcast * lax.rsqrt(mean_sq + EPSILON) * gain_vec).astype(jnp.bfloat16)


def project_heads(states, weight):
    projected = jnp.dot(states.reshape(-1, D_MODEL), weight, preferred_element_type=jnp.float32)
    return projected.astype(jnp.bfloat16).reshape(states.shape[0], states.shape[1], NUM_HEADS, HEAD_DIM)


def output_sum(context, weight):
    return jnp.dot(context.reshape(-1, HIDDEN), weight, preferred_element_type=jnp.float32)


def residual_add(states, update):
    return (states.astype(jnp.float32) + update.reshape(states.shape)).astype(jnp.bfloat16)


def softmax_mix(queries, key_heads, values, bias_mask):
    scores = jnp.einsum('qhe,khe->hqk', queries.astype(jnp.float32), key_heads.astype(jnp.float32)) + bias_mask
    weights = jax.nn.softmax(scores, axis=-1).astype(jnp.bfloat16)
    return jnp.einsum('hqk,khe->qhe', weights.astype(jnp.float32), values.astype(jnp.float32)).astype(jnp.bfloat16)


def expert_ffn(operands):
    inputs, first_w, second_w = operands
    hidden = jnp.maximum(jnp.dot(inputs, first_w, preferred_element_type=jnp.float32), 0.0).astype(jnp.bfloat16)
    return jnp.dot(hidden, second_w, preferred_element_type=jnp.float32).astype(jnp.bfloat16)


def reference(dec_states, enc_states, enc_pad, expert_idx, self_bias, gain_self, wq_self, wk_self, wv_self, wo_self, gain_cross, wq_cross, wk_cross, wv_cross, wo_cross, gain_ffn, w_router, w_in, w_out):
    row_ids = jnp.arange(DEC_LEN)[:, None]
    col_ids = jnp.arange(DEC_LEN)[None, :]
    causal_bias = jnp.where(col_ids <= row_ids, self_bias, NEG_LARGE)

    def self_seq(operands):
        return softmax_mix(operands[0], operands[1], operands[2], causal_bias)

    def cross_seq(operands):
        return softmax_mix(operands[0], operands[1], operands[2], operands[3])

    normed = rms_norm(dec_states, gain_self)
    context = lax.map(self_seq, (project_heads(normed, wq_self), project_heads(normed, wk_self), project_heads(normed, wv_self)))
    after_self = residual_add(dec_states, output_sum(context, wo_self))

    pad_bias = jnp.where(enc_pad == 0, 0.0, NEG_LARGE).astype(jnp.float32)[:, None, None, :]
    normed = rms_norm(after_self, gain_cross)
    context = lax.map(cross_seq, (project_heads(normed, wq_cross), project_heads(enc_states, wk_cross), project_heads(enc_states, wv_cross), pad_bias))
    after_cross = residual_add(after_self, output_sum(context, wo_cross))

    normed = rms_norm(after_cross, gain_ffn).reshape(GROUPS, TOKENS, D_MODEL)
    logits = jnp.dot(normed.reshape(-1, D_MODEL).astype(jnp.float32), w_router)
    router_prob = jax.nn.softmax(logits, axis=-1).reshape(GROUPS, TOKENS, EXPERTS)
    choice = expert_idx.reshape(GROUPS, TOKENS)
    one_hot = (choice[:, :, None] == jnp.arange(EXPERTS)[None, None, :]).astype(jnp.int32)
    gate_prob = jnp.sum(router_prob * one_hot, axis=-1)
    position = jnp.sum((jnp.cumsum(one_hot, axis=1) - 1) * one_hot, axis=-1)
    is_kept = position < CAPACITY
    slot_count = EXPERTS * CAPACITY
    slot_id = jnp.where(is_kept, choice * CAPACITY + position, slot_count)
    target = jnp.arange(GROUPS)[:, None] * (slot_count + 1) + slot_id
    buffers = jnp.zeros((GROUPS * (slot_count + 1), D_MODEL), jnp.bfloat16)
    buffers = buffers.at[target.reshape(-1)].set(normed.reshape(-1, D_MODEL))
    buffers = buffers.reshape(GROUPS, slot_count + 1, D_MODEL)[:, :slot_count]
    per_expert = jnp.transpose(buffers.reshape(GROUPS, EXPERTS, CAPACITY, D_MODEL), (1, 0, 2, 3)).reshape(EXPERTS, GROUPS * CAPACITY, D_MODEL)
    expert_out = lax.map(expert_ffn, (per_expert, w_in, w_out))
    expert_out = jnp.transpose(expert_out.reshape(EXPERTS, GROUPS, CAPACITY, D_MODEL), (1, 0, 2, 3)).reshape(GROUPS * slot_count, D_MODEL)
    source = jnp.arange(GROUPS)[:, None] * slot_count + jnp.where(is_kept, slot_id, 0)
    picked = expert_out[source.reshape(-1)].astype(jnp.float32).reshape(GROUPS, TOKENS, D_MODEL)
    moe_out = (gate_prob * is_kept)[:, :, None] * picked
    result = after_cross.reshape(GROUPS, TOKENS, D_MODEL).astype(jnp.float32) + moe_out
    return result.astype(jnp.bfloat16).reshape(GROUP_BATCH, DEC_LEN, D_MODEL)
```

```python
import jax
import jax.numpy as jnp
from jax import lax
from jax.sharding import PartitionSpec as P

EPSILON = 1e-6
NEG_LARGE = -1e30


def rms_norm(states, gain_vec):
    upcast = states.astype(jnp.float32)
    mean_sq = jnp.mean(upcast * upcast, axis=-1, keepdims=True)
    return (upcast * lax.rsqrt(mean_sq + EPSILON) * gain_vec).astype(jnp.bfloat16)


def matmul_f32(left, right):
    return jnp.dot(left, right, preferred_element_type=jnp.float32)


def split_heads(flat, heads):
    return flat.reshape(flat.shape[0], flat.shape[1], heads, flat.shape[2] // heads)


def attention_context(queries, key_heads, values, bias_mask):
    scores = jnp.einsum('bqhe,bkhe->bhqk', queries, key_heads, preferred_element_type=jnp.float32) + bias_mask
    weights = jax.nn.softmax(scores, axis=-1).astype(jnp.bfloat16)
    context = jnp.einsum('bhqk,bkhe->bqhe', weights, values, preferred_element_type=jnp.float32).astype(jnp.bfloat16)
    return context.reshape(context.shape[0], context.shape[1], -1)


def split_three(weight):
    high = weight.astype(jnp.bfloat16)
    rest = weight - high.astype(jnp.float32)
    mid = rest.astype(jnp.bfloat16)
    low = (rest - mid.astype(jnp.float32)).astype(jnp.bfloat16)
    return high, mid, low


def token_positions(choice, experts):
    tokens = choice.shape[0]
    block = 128
    one_hot = (choice[:, None] == lax.broadcasted_iota(jnp.int32, (tokens, experts), 1)).astype(jnp.bfloat16)
    blocks = one_hot.reshape(tokens // block, block, experts)
    lower = (lax.broadcasted_iota(jnp.int32, (block, block), 0) >= lax.broadcasted_iota(jnp.int32, (block, block), 1)).astype(jnp.bfloat16)
    inside = jnp.einsum('ij,bje->bie', lower, blocks, preferred_element_type=jnp.float32)
    totals = inside[:, -1, :]
    before = jnp.cumsum(totals, axis=0) - totals
    counts = (inside + before[:, None, :]).reshape(tokens, experts)
    return (jnp.sum(counts * one_hot.astype(jnp.float32), axis=-1) - 1.0).astype(jnp.int32)


def solution(mesh):
    ep_size = mesh.shape['ep']
    tp_size = mesh.shape['tp']
    token_spec = P(('part', 'ep'), None, None)
    row_spec = P(('part', 'ep'), None)
    col_spec = P(None, 'tp')
    head_rows = P('tp', None)
    vec_spec = P(None)
    expert_spec = P('ep', None, None)
    in_specs = (token_spec, token_spec, row_spec, row_spec, P('tp', None, None), vec_spec, col_spec, col_spec, col_spec, head_rows, vec_spec, col_spec, col_spec, col_spec, head_rows, vec_spec, P(None, None), expert_spec, expert_spec)

    def layer(dec_states, enc_states, enc_pad, expert_idx, self_bias, gain_self, wq_self, wk_self, wv_self, wo_self, gain_cross, wq_cross, wk_cross, wv_cross, wo_cross, gain_ffn, w_router, w_in, w_out):
        batch_dev, dec_len, d_model = dec_states.shape
        heads = self_bias.shape[0]
        width = wo_self.shape[0]
        own_batch = batch_dev // tp_size
        tp_id = lax.axis_index('tp')

        w_pack = jnp.concatenate([wo_self, wo_cross, wq_cross.T], axis=0)
        w_all = lax.all_gather(w_pack, 'tp', axis=0, tiled=False)
        wo_self_all = w_all[:, :width].reshape(tp_size * width, d_model)
        wo_cross_all = w_all[:, width:2 * width].reshape(tp_size * width, d_model)
        wq_cross_all = w_all[:, 2 * width:].reshape(tp_size * width, d_model)

        kv_local = jnp.concatenate([matmul_f32(enc_states, wk_cross), matmul_f32(enc_states, wv_cross)], axis=-1).astype(jnp.bfloat16)
        kv_own = lax.all_to_all(kv_local.reshape(tp_size, own_batch, -1, 2 * width), 'tp', 0, 0, tiled=True)

        row_ids = lax.broadcasted_iota(jnp.int32, (dec_len, dec_len), 0)
        col_ids = lax.broadcasted_iota(jnp.int32, (dec_len, dec_len), 1)
        causal_bias = jnp.where(col_ids <= row_ids, self_bias, NEG_LARGE)[None]
        normed = rms_norm(dec_states, gain_self)
        queries = split_heads(matmul_f32(normed, wq_self).astype(jnp.bfloat16), heads)
        key_heads = split_heads(matmul_f32(normed, wk_self).astype(jnp.bfloat16), heads)
        values = split_heads(matmul_f32(normed, wv_self).astype(jnp.bfloat16), heads)
        context = attention_context(queries, key_heads, values, causal_bias)
        context = lax.all_to_all(context, 'tp', 0, 2, tiled=True)
        dec_own = lax.dynamic_slice_in_dim(dec_states, tp_id * own_batch, own_batch, 0)
        after_self = (dec_own.astype(jnp.float32) + matmul_f32(context, wo_self_all)).astype(jnp.bfloat16)

        pad_own = lax.dynamic_slice_in_dim(enc_pad, tp_id * own_batch, own_batch, 0)
        pad_bias = jnp.where(pad_own == 0, 0.0, NEG_LARGE).astype(jnp.float32)[:, None, None, :]
        normed = rms_norm(after_self, gain_cross)
        all_heads = heads * tp_size
        queries = jnp.einsum('bld,kd->blk', normed, wq_cross_all, preferred_element_type=jnp.float32).astype(jnp.bfloat16)
        kv_own = jnp.transpose(kv_own, (1, 2, 0, 3))
        k_own = kv_own[..., :width].reshape(own_batch, -1, tp_size * width)
        v_own = kv_own[..., width:].reshape(own_batch, -1, tp_size * width)
        context = attention_context(split_heads(queries, all_heads), split_heads(k_own, all_heads), split_heads(v_own, all_heads), pad_bias)
        after_cross = (after_self.astype(jnp.float32) + matmul_f32(context, wo_cross_all)).astype(jnp.bfloat16)
        after_cross = lax.all_gather(after_cross, 'tp', axis=0, tiled=True)

        tokens = batch_dev * dec_len
        experts = w_router.shape[1]
        capacity = (5 * tokens + 4 * experts - 1) // (4 * experts)
        row_cap = -(-capacity // tp_size)
        slots = experts * row_cap
        choice = expert_idx.reshape(tokens)
        position = token_positions(choice, experts)
        kept = position < capacity
        slot_row = position // row_cap
        local_slot = choice * row_cap + position % row_cap
        slot_here = jnp.where(kept & (slot_row == tp_id), local_slot, -1)
        slot_full = jnp.where(kept, slot_row * slots + local_slot, -1)

        states = after_cross.reshape(tokens, d_model)
        normed = rms_norm(states, gain_ffn)
        dispatch = (lax.broadcasted_iota(jnp.int32, (slots, tokens), 0) == slot_here[None, :]).astype(jnp.bfloat16)
        send_buf = matmul_f32(dispatch, normed).astype(jnp.bfloat16)
        local_experts = experts // ep_size
        received = lax.all_to_all(send_buf.reshape(ep_size, local_experts * row_cap, d_model), 'ep', 0, 0, tiled=True)
        received = received.reshape(ep_size, local_experts, row_cap, d_model)
        received = jnp.transpose(received, (1, 0, 2, 3)).reshape(local_experts, ep_size * row_cap, d_model)
        hidden = jnp.maximum(jnp.einsum('ecd,edf->ecf', received, w_in, preferred_element_type=jnp.float32), 0.0).astype(jnp.bfloat16)
        expert_out = jnp.einsum('ecf,efd->ecd', hidden, w_out, preferred_element_type=jnp.float32).astype(jnp.bfloat16)
        expert_out = jnp.transpose(expert_out.reshape(local_experts, ep_size, row_cap, d_model), (1, 0, 2, 3))
        returned = lax.all_to_all(expert_out.reshape(ep_size, local_experts * row_cap, d_model), 'ep', 0, 0, tiled=True)
        all_slots = lax.all_gather(returned.reshape(slots, d_model), 'tp', axis=0, tiled=True)

        logits = sum(matmul_f32(normed, piece) for piece in split_three(w_router))
        router_prob = jax.nn.softmax(logits, axis=-1)
        gate_prob = jnp.sum(jnp.where(choice[:, None] == lax.broadcasted_iota(jnp.int32, (tokens, experts), 1), router_prob, 0.0), axis=-1)
        pick = (slot_full[:, None] == lax.broadcasted_iota(jnp.int32, (tokens, tp_size * slots), 1)).astype(jnp.bfloat16)
        combined = matmul_f32(pick, all_slots)
        result = states.astype(jnp.float32) + gate_prob[:, None] * combined
        return result.astype(jnp.bfloat16).reshape(batch_dev, dec_len, d_model)

    return jax.shard_map(layer, mesh=mesh, in_specs=in_specs, out_specs=token_spec, check_vma=False)
```

```python
import functools
import jax
import jax.numpy as jnp
from jax import lax
from jax.experimental import pallas as pl
from jax.experimental.pallas import tpu as pltpu
from jax.sharding import PartitionSpec as P

EPSILON = 1e-6
NEG_LARGE = -1e30


def rms_norm(states, gain_vec):
    upcast = states.astype(jnp.float32)
    mean_sq = jnp.mean(upcast * upcast, axis=-1, keepdims=True)
    return (upcast * lax.rsqrt(mean_sq + EPSILON) * gain_vec).astype(jnp.bfloat16)


def matmul_f32(left, right):
    return jnp.dot(left, right, preferred_element_type=jnp.float32)


def split_heads(flat, heads):
    return flat.reshape(flat.shape[0], flat.shape[1], heads, flat.shape[2] // heads)


def attention_context(queries, key_heads, values, bias_mask):
    scores = jnp.einsum('bqhe,bkhe->bhqk', queries, key_heads, preferred_element_type=jnp.float32) + bias_mask
    weights = jax.nn.softmax(scores, axis=-1).astype(jnp.bfloat16)
    context = jnp.einsum('bhqk,bkhe->bqhe', weights, values, preferred_element_type=jnp.float32).astype(jnp.bfloat16)
    return context.reshape(context.shape[0], context.shape[1], -1)


def split_three(weight):
    high = weight.astype(jnp.bfloat16)
    rest = weight - high.astype(jnp.float32)
    mid = rest.astype(jnp.bfloat16)
    low = (rest - mid.astype(jnp.float32)).astype(jnp.bfloat16)
    return high, mid, low


def token_positions(choice, experts):
    tokens = choice.shape[0]
    block = 128
    one_hot = (choice[:, None] == lax.broadcasted_iota(jnp.int32, (tokens, experts), 1)).astype(jnp.bfloat16)
    blocks = one_hot.reshape(tokens // block, block, experts)
    lower = (lax.broadcasted_iota(jnp.int32, (block, block), 0) >= lax.broadcasted_iota(jnp.int32, (block, block), 1)).astype(jnp.bfloat16)
    inside = jnp.einsum('ij,bje->bie', lower, blocks, preferred_element_type=jnp.float32)
    totals = inside[:, -1, :]
    before = jnp.cumsum(totals, axis=0) - totals
    counts = (inside + before[:, None, :]).reshape(tokens, experts)
    return (jnp.sum(counts * one_hot.astype(jnp.float32), axis=-1) - 1.0).astype(jnp.int32)


MESH_ID = pl.DeviceIdType.MESH


def expert_kernel(ep_size, tp_size, send_ref, states_ref, code_ref, gate_ref, w_in_ref, w_out_ref, out_ref, w_in_buf, w_out_buf, recv_buf, hidden_buf, out_buf, slot_buf, w_sem, disp_send, disp_recv, back_send, back_recv, near_send, near_recv, far_send, far_recv):
    me = lax.axis_index('ep')
    row = lax.axis_index('tp')
    chips = ep_size // 2
    chip = me // 2
    partner = me + 1 - 2 * (me % 2)
    above = (row + 1) % tp_size
    below = (row + tp_size - 1) % tp_size
    across = (row + 2) % tp_size
    capacity, d_model = send_ref.shape[1], send_ref.shape[2]
    d_ff = w_in_buf.shape[1]
    pair = 2 * capacity
    tokens = states_ref.shape[0]

    def weight_copies():
        return (pltpu.make_async_copy(w_in_ref.at[row], w_in_buf, w_sem.at[0]),
                pltpu.make_async_copy(w_out_ref.at[row], w_out_buf, w_sem.at[1]))

    copy_in, copy_out = weight_copies()
    copy_in.start()
    copy_out.start()

    barrier = pltpu.get_barrier_semaphore()
    for step in range(1, ep_size):
        pl.semaphore_signal(barrier, inc=1, device_id={'ep': (me + step) % ep_size}, device_id_type=MESH_ID)
    for neighbour in (above, below):
        pl.semaphore_signal(barrier, inc=1, device_id={'tp': neighbour}, device_id_type=MESH_ID)
    pl.semaphore_wait(barrier, ep_size + 1)

    def peers(relative):
        if relative == 0:
            return (partner,)
        first = 2 * ((chip + relative) % chips)
        return (first, first + 1)

    def dispatch_copy(peer, source):
        return pltpu.make_async_remote_copy(
            src_ref=send_ref.at[peer], dst_ref=recv_buf.at[source], send_sem=disp_send.at[peer], recv_sem=disp_recv.at[source],
            device_id={'ep': peer}, device_id_type=MESH_ID)

    def back_copy(peer, source):
        return pltpu.make_async_remote_copy(
            src_ref=out_buf.at[peer], dst_ref=slot_buf.at[row, source], send_sem=back_send.at[peer], recv_sem=back_recv.at[source],
            device_id={'ep': peer}, device_id_type=MESH_ID)

    def near_copy(relative, holder, side, target):
        block = 2 * ((chip + relative) % chips)
        return pltpu.make_async_remote_copy(
            src_ref=slot_buf.at[holder, pl.ds(block, 2)], dst_ref=slot_buf.at[holder, pl.ds(block, 2)],
            send_sem=near_send.at[relative, side], recv_sem=near_recv.at[relative, side],
            device_id={'tp': target}, device_id_type=MESH_ID)

    def far_copy(relative, holder, side, target):
        block = 2 * ((chip + relative) % chips) + side
        return pltpu.make_async_remote_copy(
            src_ref=slot_buf.at[holder, block], dst_ref=slot_buf.at[holder, block],
            send_sem=far_send.at[relative, side], recv_sem=far_recv.at[relative, side],
            device_id={'tp': target}, device_id_type=MESH_ID)

    compute_order = (0, 1, chips - 1, 2)
    back_order = (0, chips - 1, 1, 2)
    for relative in compute_order:
        for peer in peers(relative):
            dispatch_copy(peer, me).start()
    recv_buf[me] = send_ref[me]
    out_ref[...] = states_ref[...]

    def compute(relative):
        for peer in peers(relative):
            dispatch_copy(peer, peer).wait_recv()
        if relative == 0:
            copy_in.wait()
        block = 2 * ((chip + relative) % chips)
        inputs = recv_buf[pl.ds(block, 2)].reshape(pair, d_model)
        width = d_ff // 4

        def first(step, carry):
            columns = pl.ds(pl.multiple_of(step * width, width), width)
            hidden = jnp.dot(inputs, w_in_buf[:, columns], preferred_element_type=jnp.float32)
            hidden_buf[:, columns] = jnp.maximum(hidden, 0.0).astype(jnp.bfloat16)
            return carry

        lax.fori_loop(0, 4, first, 0)
        if relative == 0:
            copy_out.wait()
        result = jnp.dot(hidden_buf[...], w_out_buf[...], preferred_element_type=jnp.float32).astype(jnp.bfloat16)
        out_buf[pl.ds(block, 2)] = result.reshape(2, capacity, d_model)
        if relative == 0:
            slot_buf[row, me] = out_buf[me]
        for peer in peers(relative):
            back_copy(peer, me).start()

    def share(relative):
        for peer in peers(relative):
            back_copy(peer, peer).wait_recv()
        near_copy(relative, row, 0, above).start()
        near_copy(relative, row, 1, below).start()

    def forward(relative):
        near_copy(relative, below, 0, above).wait_recv()
        far_copy(relative, below, 0, above).start()
        near_copy(relative, above, 1, below).wait_recv()
        far_copy(relative, above, 1, below).start()

    def combine(relative):
        far_copy(relative, across, 0, above).wait_recv()
        far_copy(relative, across, 1, below).wait_recv()
        which = (chip + relative) % chips
        values = jnp.concatenate([slot_buf[holder, pl.ds(2 * which, 2)].reshape(pair, d_model) for holder in range(tp_size)], axis=0)
        tile = 256

        def body(step, carry):
            rows = pl.ds(pl.multiple_of(step * tile, tile), tile)
            wanted = code_ref[rows, :] - which * (tp_size * pair)
            pick = (wanted == lax.broadcasted_iota(jnp.int32, (tile, tp_size * pair), 1)).astype(jnp.float32).astype(jnp.bfloat16)
            picked = jnp.dot(pick, values, preferred_element_type=jnp.float32)
            out_ref[rows, :] = (out_ref[rows, :].astype(jnp.float32) + gate_ref[rows, :] * picked).astype(jnp.bfloat16)
            return carry

        lax.fori_loop(0, tokens // tile, body, 0)

    near_1, near_2, near_3 = back_order[1:]
    compute(compute_order[0])
    share(0)
    compute(compute_order[1])
    compute(compute_order[2])
    share(near_1)
    forward(0)
    compute(compute_order[3])
    share(near_2)
    forward(near_1)
    combine(0)
    share(near_3)
    forward(near_2)
    combine(near_1)
    forward(near_3)
    combine(near_2)
    combine(near_3)

    for relative in compute_order:
        for peer in peers(relative):
            dispatch_copy(peer, me).wait_send()
            back_copy(peer, me).wait_send()
        near_copy(relative, row, 0, above).wait_send()
        near_copy(relative, row, 1, below).wait_send()
        far_copy(relative, below, 0, above).wait_send()
        far_copy(relative, above, 1, below).wait_send()


def expert_exchange(send_buf, states, code, gate, w_in, w_out, ep_size, tp_size):
    capacity, d_model = send_buf.shape[1], send_buf.shape[2]
    d_ff = w_in.shape[2]
    vmem = pl.BlockSpec(memory_space=pltpu.VMEM)
    anywhere = pl.BlockSpec(memory_space=pl.ANY)
    dma = pltpu.SemaphoreType.DMA
    chips = ep_size // 2
    return pl.pallas_call(
        functools.partial(expert_kernel, ep_size, tp_size),
        out_shape=jax.ShapeDtypeStruct(states.shape, jnp.bfloat16),
        in_specs=[vmem, vmem, vmem, vmem, anywhere, anywhere],
        out_specs=vmem,
        scratch_shapes=[
            pltpu.VMEM((d_model, d_ff), jnp.bfloat16),
            pltpu.VMEM((d_ff, d_model), jnp.bfloat16),
            pltpu.VMEM((ep_size, capacity, d_model), jnp.bfloat16),
            pltpu.VMEM((2 * capacity, d_ff), jnp.bfloat16),
            pltpu.VMEM((ep_size, capacity, d_model), jnp.bfloat16),
            pltpu.VMEM((tp_size, ep_size, capacity, d_model), jnp.bfloat16),
            dma((2,)), dma((ep_size,)), dma((ep_size,)), dma((ep_size,)), dma((ep_size,)),
            dma((chips, 2)), dma((chips, 2)), dma((chips, 2)), dma((chips, 2)),
        ],
        compiler_params=pltpu.CompilerParams(collective_id=0, has_side_effects=True),
        name='expert_exchange',
    )(send_buf, states, code, gate, w_in, w_out)


def solution(mesh):
    ep_size = mesh.shape['ep']
    tp_size = mesh.shape['tp']
    token_spec = P(('part', 'ep'), None, None)
    row_spec = P(('part', 'ep'), None)
    col_spec = P(None, 'tp')
    head_rows = P('tp', None)
    vec_spec = P(None)
    expert_spec = P('ep', None, None)
    in_specs = (token_spec, token_spec, row_spec, row_spec, P('tp', None, None), vec_spec, col_spec, col_spec, col_spec, head_rows, vec_spec, col_spec, col_spec, col_spec, head_rows, vec_spec, P(None, None), expert_spec, expert_spec)

    def layer(dec_states, enc_states, enc_pad, expert_idx, self_bias, gain_self, wq_self, wk_self, wv_self, wo_self, gain_cross, wq_cross, wk_cross, wv_cross, wo_cross, gain_ffn, w_router, w_in, w_out):
        batch_dev, dec_len, d_model = dec_states.shape
        heads = self_bias.shape[0]
        width = wo_self.shape[0]
        own_batch = batch_dev // tp_size
        tp_id = lax.axis_index('tp')

        w_pack = jnp.concatenate([wo_self, wo_cross, wq_cross.T], axis=0)
        w_all = lax.all_gather(w_pack, 'tp', axis=0, tiled=False)
        wo_self_all = w_all[:, :width].reshape(tp_size * width, d_model)
        wo_cross_all = w_all[:, width:2 * width].reshape(tp_size * width, d_model)
        wq_cross_all = w_all[:, 2 * width:].reshape(tp_size * width, d_model)

        kv_local = jnp.concatenate([matmul_f32(enc_states, wk_cross), matmul_f32(enc_states, wv_cross)], axis=-1).astype(jnp.bfloat16)
        kv_own = lax.all_to_all(kv_local.reshape(tp_size, own_batch, -1, 2 * width), 'tp', 0, 0, tiled=True)

        row_ids = lax.broadcasted_iota(jnp.int32, (dec_len, dec_len), 0)
        col_ids = lax.broadcasted_iota(jnp.int32, (dec_len, dec_len), 1)
        causal_bias = jnp.where(col_ids <= row_ids, self_bias, NEG_LARGE)[None]
        normed = rms_norm(dec_states, gain_self)
        queries = split_heads(matmul_f32(normed, wq_self).astype(jnp.bfloat16), heads)
        key_heads = split_heads(matmul_f32(normed, wk_self).astype(jnp.bfloat16), heads)
        values = split_heads(matmul_f32(normed, wv_self).astype(jnp.bfloat16), heads)
        context = attention_context(queries, key_heads, values, causal_bias)
        context = lax.all_to_all(context, 'tp', 0, 2, tiled=True)
        dec_own = lax.dynamic_slice_in_dim(dec_states, tp_id * own_batch, own_batch, 0)
        after_self = (dec_own.astype(jnp.float32) + matmul_f32(context, wo_self_all)).astype(jnp.bfloat16)

        pad_own = lax.dynamic_slice_in_dim(enc_pad, tp_id * own_batch, own_batch, 0)
        pad_bias = jnp.where(pad_own == 0, 0.0, NEG_LARGE).astype(jnp.float32)[:, None, None, :]
        normed = rms_norm(after_self, gain_cross)
        all_heads = heads * tp_size
        queries = jnp.einsum('bld,kd->blk', normed, wq_cross_all, preferred_element_type=jnp.float32).astype(jnp.bfloat16)
        kv_own = jnp.transpose(kv_own, (1, 2, 0, 3))
        k_own = kv_own[..., :width].reshape(own_batch, -1, tp_size * width)
        v_own = kv_own[..., width:].reshape(own_batch, -1, tp_size * width)
        context = attention_context(split_heads(queries, all_heads), split_heads(k_own, all_heads), split_heads(v_own, all_heads), pad_bias)
        after_cross = (after_self.astype(jnp.float32) + matmul_f32(context, wo_cross_all)).astype(jnp.bfloat16)
        after_cross = lax.all_gather(after_cross, 'tp', axis=0, tiled=True)

        tokens = batch_dev * dec_len
        experts = w_router.shape[1]
        capacity = (5 * tokens + 4 * experts - 1) // (4 * experts)
        local_experts = experts // ep_size
        assert local_experts == tp_size
        choice = expert_idx.reshape(tokens)
        position = token_positions(choice, experts)
        kept = position < capacity
        owner = choice // local_experts
        owner_row = choice % local_experts
        slots = ep_size * capacity
        slot_here = jnp.where(kept & (owner_row == tp_id), owner * capacity + position, -1)
        pair_slots = 2 * capacity
        code = (owner // 2) * (tp_size * pair_slots) + owner_row * pair_slots + (owner % 2) * capacity + position
        code = jnp.where(kept, code, -1)

        states = after_cross.reshape(tokens, d_model)
        normed = rms_norm(states, gain_ffn)
        dispatch = (lax.broadcasted_iota(jnp.int32, (slots, tokens), 0) == slot_here[None, :]).astype(jnp.bfloat16)
        send_buf = matmul_f32(dispatch, normed).astype(jnp.bfloat16).reshape(ep_size, capacity, d_model)

        logits = sum(matmul_f32(normed, piece) for piece in split_three(w_router))
        router_prob = jax.nn.softmax(logits, axis=-1)
        gate_prob = jnp.sum(jnp.where(choice[:, None] == lax.broadcasted_iota(jnp.int32, (tokens, experts), 1), router_prob, 0.0), axis=-1)
        result = expert_exchange(send_buf, states, code[:, None], gate_prob[:, None], w_in, w_out, ep_size, tp_size)
        return result.reshape(batch_dev, dec_len, d_model)

    return jax.shard_map(layer, mesh=mesh, in_specs=in_specs, out_specs=token_spec, check_vma=False)
```

```python
import functools
import jax
import jax.numpy as jnp
from jax import lax
from jax.experimental import pallas as pl
from jax.experimental.pallas import tpu as pltpu
from jax.sharding import PartitionSpec as P

EPSILON = 1e-6
NEG_LARGE = -1e30


def rms_norm(states, gain_vec):
    upcast = states.astype(jnp.float32)
    mean_sq = jnp.mean(upcast * upcast, axis=-1, keepdims=True)
    return (upcast * lax.rsqrt(mean_sq + EPSILON) * gain_vec).astype(jnp.bfloat16)


def matmul_f32(left, right):
    return jnp.dot(left, right, preferred_element_type=jnp.float32)


def split_heads(flat, heads):
    return flat.reshape(flat.shape[0], flat.shape[1], heads, flat.shape[2] // heads)


def attention_context(queries, key_heads, values, bias_mask):
    scores = jnp.einsum('bqhe,bkhe->bhqk', queries, key_heads, preferred_element_type=jnp.float32) + bias_mask
    weights = jax.nn.softmax(scores, axis=-1).astype(jnp.bfloat16)
    context = jnp.einsum('bhqk,bkhe->bqhe', weights, values, preferred_element_type=jnp.float32).astype(jnp.bfloat16)
    return context.reshape(context.shape[0], context.shape[1], -1)


def split_three(weight):
    high = weight.astype(jnp.bfloat16)
    rest = weight - high.astype(jnp.float32)
    mid = rest.astype(jnp.bfloat16)
    low = (rest - mid.astype(jnp.float32)).astype(jnp.bfloat16)
    return high, mid, low


def token_positions(choice, experts):
    tokens = choice.shape[0]
    block = 128
    one_hot = (choice[:, None] == lax.broadcasted_iota(jnp.int32, (tokens, experts), 1)).astype(jnp.bfloat16)
    blocks = one_hot.reshape(tokens // block, block, experts)
    lower = (lax.broadcasted_iota(jnp.int32, (block, block), 0) >= lax.broadcasted_iota(jnp.int32, (block, block), 1)).astype(jnp.bfloat16)
    inside = jnp.einsum('ij,bje->bie', lower, blocks, preferred_element_type=jnp.float32)
    totals = inside[:, -1, :]
    before = jnp.cumsum(totals, axis=0) - totals
    counts = (inside + before[:, None, :]).reshape(tokens, experts)
    return (jnp.sum(counts * one_hot.astype(jnp.float32), axis=-1) - 1.0).astype(jnp.int32)


MESH_ID = pl.DeviceIdType.MESH


def expert_kernel(ep_size, tp_size, capacity, experts, own_ref, slot_ref, code_ref, gain_ref, route_ref, w_in_ref, w_out_ref, out_ref, w_in_buf, w_out_buf, states_buf, gate_buf, send_ref, recv_buf, hidden_buf, out_buf, slot_buf, w_sem, part_send, part_recv, rest_send, rest_recv, disp_send, disp_recv, back_send, back_recv, near_send, near_recv, far_send, far_recv):
    me = lax.axis_index('ep')
    row = lax.axis_index('tp')
    chips = ep_size // 2
    chip = me // 2
    partner = me + 1 - 2 * (me % 2)
    above = (row + 1) % tp_size
    below = (row + tp_size - 1) % tp_size
    across = (row + 2) % tp_size
    own_batch, dec_len, d_model = own_ref.shape
    d_ff = w_in_buf.shape[1]
    pair = 2 * capacity
    tokens = code_ref.shape[0]
    slots = ep_size * capacity
    lanes = 128

    def weight_copies():
        return (pltpu.make_async_copy(w_in_ref.at[row], w_in_buf, w_sem.at[0]),
                pltpu.make_async_copy(w_out_ref.at[row], w_out_buf, w_sem.at[1]))

    copy_in, copy_out = weight_copies()
    copy_in.start()
    copy_out.start()

    barrier = pltpu.get_barrier_semaphore()
    for step in range(1, ep_size):
        pl.semaphore_signal(barrier, inc=1, device_id={'ep': (me + step) % ep_size}, device_id_type=MESH_ID)
    for neighbour in (above, below):
        pl.semaphore_signal(barrier, inc=1, device_id={'tp': neighbour}, device_id_type=MESH_ID)
    pl.semaphore_wait(barrier, ep_size + 1)

    def peers(relative):
        if relative == 0:
            return (partner,)
        first = 2 * ((chip + relative) % chips)
        return (first, first + 1)

    def dispatch_copy(peer, source):
        return pltpu.make_async_remote_copy(
            src_ref=send_ref.at[peer], dst_ref=recv_buf.at[source], send_sem=disp_send.at[peer], recv_sem=disp_recv.at[source],
            device_id={'ep': peer}, device_id_type=MESH_ID)

    def back_copy(peer, source):
        return pltpu.make_async_remote_copy(
            src_ref=out_buf.at[peer], dst_ref=slot_buf.at[row, source], send_sem=back_send.at[peer], recv_sem=back_recv.at[source],
            device_id={'ep': peer}, device_id_type=MESH_ID)

    def near_copy(relative, holder, side, target):
        block = 2 * ((chip + relative) % chips)
        return pltpu.make_async_remote_copy(
            src_ref=slot_buf.at[holder, pl.ds(block, 2)], dst_ref=slot_buf.at[holder, pl.ds(block, 2)],
            send_sem=near_send.at[relative, side], recv_sem=near_recv.at[relative, side],
            device_id={'tp': target}, device_id_type=MESH_ID)

    def far_copy(relative, holder, side, target):
        block = 2 * ((chip + relative) % chips) + side
        return pltpu.make_async_remote_copy(
            src_ref=slot_buf.at[holder, block], dst_ref=slot_buf.at[holder, block],
            send_sem=far_send.at[relative, side], recv_sem=far_recv.at[relative, side],
            device_id={'tp': target}, device_id_type=MESH_ID)

    def part_copy(holder, part, side, target):
        source = own_ref.at[part] if holder is row else states_buf.at[holder, part]
        return pltpu.make_async_remote_copy(
            src_ref=source, dst_ref=states_buf.at[holder, part], send_sem=part_send.at[part, side], recv_sem=part_recv.at[part, side],
            device_id={'tp': target}, device_id_type=MESH_ID)

    def rest_copy(holder, side, target):
        return pltpu.make_async_remote_copy(
            src_ref=states_buf.at[holder, side], dst_ref=states_buf.at[holder, side], send_sem=rest_send.at[side], recv_sem=rest_recv.at[side],
            device_id={'tp': target}, device_id_type=MESH_ID)

    part_copy(row, 0, 0, above).start()
    part_copy(row, 1, 1, below).start()
    part_copy(row, 1, 0, above).start()
    part_copy(row, 0, 1, below).start()
    states_buf[row] = own_ref[...]
    lane_ids = lax.broadcasted_iota(jnp.int32, (1, lanes), 1)
    local = experts // ep_size
    owner = lane_ids // local
    base = (owner // 2) * (tp_size * pair) + (lane_ids % local) * pair + (owner % 2) * capacity

    def absorb(holder, part, fresh):
        block = holder * own_batch + part
        upcast = states_buf[holder, part].astype(jnp.float32)
        mean_sq = jnp.mean(upcast * upcast, axis=-1, keepdims=True)
        normed = (upcast * lax.rsqrt(mean_sq + EPSILON) * gain_ref[...]).astype(jnp.bfloat16)
        wanted = slot_ref[block]
        pick = (wanted == lax.broadcasted_iota(jnp.int32, (slots, dec_len), 0)).astype(jnp.float32).astype(jnp.bfloat16)
        picked = jnp.dot(pick, normed, preferred_element_type=jnp.float32).astype(jnp.bfloat16).reshape(ep_size, capacity, d_model)
        if fresh:
            send_ref[...] = picked
        else:
            send_ref[...] = send_ref[...] + picked
        parts = jnp.dot(normed, route_ref[...], preferred_element_type=jnp.float32)
        logits = parts[:, :lanes] + parts[:, lanes:2 * lanes] + parts[:, 2 * lanes:]
        logits = jnp.where(lane_ids < experts, logits, NEG_LARGE)
        powers = jnp.exp(logits - jnp.max(logits, axis=-1, keepdims=True))
        rows = pl.ds(pl.multiple_of(block * dec_len, dec_len), dec_len)
        place = code_ref[rows, :] - base
        chosen = (place >= 0) & (place < capacity) & (lane_ids < experts)
        gate_buf[rows, :] = jnp.sum(jnp.where(chosen, powers, 0.0), axis=-1, keepdims=True) / jnp.sum(powers, axis=-1, keepdims=True)

    def absorb_pair(first, second):
        def body(step, carry):
            absorb((row + first[0] + step * (second[0] - first[0])) % tp_size, first[1] + step * (second[1] - first[1]), False)
            return carry
        lax.fori_loop(0, 2, body, 0)

    absorb(row, 0, True)
    absorb(row, 1, False)
    part_copy(below, 0, 0, above).wait_recv()
    rest_copy(below, 0, above).start()
    part_copy(above, 1, 1, below).wait_recv()
    rest_copy(above, 1, below).start()
    absorb_pair((tp_size - 1, 0), (tp_size + 1, 1))
    part_copy(below, 1, 0, above).wait_recv()
    part_copy(above, 0, 1, below).wait_recv()
    absorb_pair((tp_size - 1, 1), (tp_size + 1, 0))
    rest_copy(across, 0, above).wait_recv()
    rest_copy(across, 1, below).wait_recv()
    absorb_pair((2, 0), (2, 1))

    compute_order = (0, 1, chips - 1, 2)
    back_order = (0, chips - 1, 1, 2)
    for relative in compute_order:
        for peer in peers(relative):
            dispatch_copy(peer, me).start()
    recv_buf[me] = send_ref[me]

    def compute(relative):
        for peer in peers(relative):
            dispatch_copy(peer, peer).wait_recv()
        if relative == 0:
            copy_in.wait()
        block = 2 * ((chip + relative) % chips)
        inputs = recv_buf[pl.ds(block, 2)].reshape(pair, d_model)
        width = d_ff // 4

        def first(step, carry):
            columns = pl.ds(pl.multiple_of(step * width, width), width)
            hidden = jnp.dot(inputs, w_in_buf[:, columns], preferred_element_type=jnp.float32)
            hidden_buf[:, columns] = jnp.maximum(hidden, 0.0).astype(jnp.bfloat16)
            return carry

        lax.fori_loop(0, 4, first, 0)
        if relative == 0:
            copy_out.wait()
        result = jnp.dot(hidden_buf[...], w_out_buf[...], preferred_element_type=jnp.float32).astype(jnp.bfloat16)
        out_buf[pl.ds(block, 2)] = result.reshape(2, capacity, d_model)
        if relative == 0:
            slot_buf[row, me] = out_buf[me]
        for peer in peers(relative):
            back_copy(peer, me).start()

    def share(relative):
        for peer in peers(relative):
            back_copy(peer, peer).wait_recv()
        near_copy(relative, row, 0, above).start()
        near_copy(relative, row, 1, below).start()

    def forward(relative):
        near_copy(relative, below, 0, above).wait_recv()
        far_copy(relative, below, 0, above).start()
        near_copy(relative, above, 1, below).wait_recv()
        far_copy(relative, above, 1, below).start()

    def combine(relative, fresh):
        far_copy(relative, across, 0, above).wait_recv()
        far_copy(relative, across, 1, below).wait_recv()
        which = (chip + relative) % chips
        values = jnp.concatenate([slot_buf[holder, pl.ds(2 * which, 2)].reshape(pair, d_model) for holder in range(tp_size)], axis=0)
        tile = dec_len

        def body(step, carry):
            previous = states_buf[step // own_batch, step % own_batch] if fresh else out_ref[pl.ds(pl.multiple_of(step * tile, tile), tile), :]
            rows = pl.ds(pl.multiple_of(step * tile, tile), tile)
            wanted = code_ref[rows, :] - which * (tp_size * pair)
            pick = (wanted == lax.broadcasted_iota(jnp.int32, (tile, tp_size * pair), 1)).astype(jnp.float32).astype(jnp.bfloat16)
            picked = jnp.dot(pick, values, preferred_element_type=jnp.float32)
            out_ref[rows, :] = (previous.astype(jnp.float32) + gate_buf[rows, :] * picked).astype(jnp.bfloat16)
            return carry

        lax.fori_loop(0, tokens // tile, body, 0)

    near_1, near_2, near_3 = back_order[1:]
    compute(compute_order[0])
    share(0)
    compute(compute_order[1])
    compute(compute_order[2])
    share(near_1)
    forward(0)
    compute(compute_order[3])
    share(near_2)
    forward(near_1)
    combine(0, True)
    share(near_3)
    forward(near_2)
    combine(near_1, False)
    forward(near_3)
    combine(near_2, False)
    combine(near_3, False)

    for part in (0, 1):
        part_copy(row, part, 0, above).wait_send()
        part_copy(row, part, 1, below).wait_send()
    rest_copy(below, 0, above).wait_send()
    rest_copy(above, 1, below).wait_send()
    for relative in compute_order:
        for peer in peers(relative):
            dispatch_copy(peer, me).wait_send()
            back_copy(peer, me).wait_send()
        near_copy(relative, row, 0, above).wait_send()
        near_copy(relative, row, 1, below).wait_send()
        far_copy(relative, below, 0, above).wait_send()
        far_copy(relative, above, 1, below).wait_send()


def expert_exchange(own, slot_here, code, gain, w_route, w_in, w_out, capacity, experts, ep_size, tp_size):
    d_model = own.shape[2]
    d_ff = w_in.shape[2]
    vmem = pl.BlockSpec(memory_space=pltpu.VMEM)
    anywhere = pl.BlockSpec(memory_space=pl.ANY)
    dma = pltpu.SemaphoreType.DMA
    chips = ep_size // 2
    return pl.pallas_call(
        functools.partial(expert_kernel, ep_size, tp_size, capacity, experts),
        out_shape=jax.ShapeDtypeStruct((code.shape[0], d_model), jnp.bfloat16),
        in_specs=[vmem, vmem, vmem, vmem, vmem, anywhere, anywhere],
        out_specs=vmem,
        scratch_shapes=[
            pltpu.VMEM((d_model, d_ff), jnp.bfloat16),
            pltpu.VMEM((d_ff, d_model), jnp.bfloat16),
            pltpu.VMEM((tp_size,) + own.shape, jnp.bfloat16),
            pltpu.VMEM((code.shape[0], 1), jnp.float32),
            pltpu.VMEM((ep_size, capacity, d_model), jnp.bfloat16),
            pltpu.VMEM((ep_size, capacity, d_model), jnp.bfloat16),
            pltpu.VMEM((2 * capacity, d_ff), jnp.bfloat16),
            pltpu.VMEM((ep_size, capacity, d_model), jnp.bfloat16),
            pltpu.VMEM((tp_size, ep_size, capacity, d_model), jnp.bfloat16),
            dma((2,)), dma((2, 2)), dma((2, 2)), dma((2,)), dma((2,)),
            dma((ep_size,)), dma((ep_size,)), dma((ep_size,)), dma((ep_size,)),
            dma((chips, 2)), dma((chips, 2)), dma((chips, 2)), dma((chips, 2)),
        ],
        compiler_params=pltpu.CompilerParams(collective_id=0, has_side_effects=True),
        name='expert_exchange',
    )(own, slot_here, code, gain, w_route, w_in, w_out)


def solution(mesh):
    ep_size = mesh.shape['ep']
    tp_size = mesh.shape['tp']
    token_spec = P(('part', 'ep'), None, None)
    row_spec = P(('part', 'ep'), None)
    col_spec = P(None, 'tp')
    head_rows = P('tp', None)
    vec_spec = P(None)
    expert_spec = P('ep', None, None)
    in_specs = (token_spec, token_spec, row_spec, row_spec, P('tp', None, None), vec_spec, col_spec, col_spec, col_spec, head_rows, vec_spec, col_spec, col_spec, col_spec, head_rows, vec_spec, P(None, None), expert_spec, expert_spec)

    def layer(dec_states, enc_states, enc_pad, expert_idx, self_bias, gain_self, wq_self, wk_self, wv_self, wo_self, gain_cross, wq_cross, wk_cross, wv_cross, wo_cross, gain_ffn, w_router, w_in, w_out):
        batch_dev, dec_len, d_model = dec_states.shape
        heads = self_bias.shape[0]
        width = wo_self.shape[0]
        own_batch = batch_dev // tp_size
        tp_id = lax.axis_index('tp')

        w_pack = jnp.concatenate([wo_self, wo_cross, wq_cross.T], axis=0)
        w_all = lax.all_gather(w_pack, 'tp', axis=0, tiled=False)
        wo_self_all = w_all[:, :width].reshape(tp_size * width, d_model)
        wo_cross_all = w_all[:, width:2 * width].reshape(tp_size * width, d_model)
        wq_cross_all = w_all[:, 2 * width:].reshape(tp_size * width, d_model)

        kv_local = jnp.concatenate([matmul_f32(enc_states, wk_cross), matmul_f32(enc_states, wv_cross)], axis=-1).astype(jnp.bfloat16)
        kv_own = lax.all_to_all(kv_local.reshape(tp_size, own_batch, -1, 2 * width), 'tp', 0, 0, tiled=True)

        row_ids = lax.broadcasted_iota(jnp.int32, (dec_len, dec_len), 0)
        col_ids = lax.broadcasted_iota(jnp.int32, (dec_len, dec_len), 1)
        causal_bias = jnp.where(col_ids <= row_ids, self_bias, NEG_LARGE)[None]
        normed = rms_norm(dec_states, gain_self)
        queries = split_heads(matmul_f32(normed, wq_self).astype(jnp.bfloat16), heads)
        key_heads = split_heads(matmul_f32(normed, wk_self).astype(jnp.bfloat16), heads)
        values = split_heads(matmul_f32(normed, wv_self).astype(jnp.bfloat16), heads)
        context = attention_context(queries, key_heads, values, causal_bias)
        context = lax.all_to_all(context, 'tp', 0, 2, tiled=True)
        dec_own = lax.dynamic_slice_in_dim(dec_states, tp_id * own_batch, own_batch, 0)
        after_self = (dec_own.astype(jnp.float32) + matmul_f32(context, wo_self_all)).astype(jnp.bfloat16)

        pad_own = lax.dynamic_slice_in_dim(enc_pad, tp_id * own_batch, own_batch, 0)
        pad_bias = jnp.where(pad_own == 0, 0.0, NEG_LARGE).astype(jnp.float32)[:, None, None, :]
        normed = rms_norm(after_self, gain_cross)
        all_heads = heads * tp_size
        queries = jnp.einsum('bld,kd->blk', normed, wq_cross_all, preferred_element_type=jnp.float32).astype(jnp.bfloat16)
        kv_own = jnp.transpose(kv_own, (1, 2, 0, 3))
        k_own = kv_own[..., :width].reshape(own_batch, -1, tp_size * width)
        v_own = kv_own[..., width:].reshape(own_batch, -1, tp_size * width)
        context = attention_context(split_heads(queries, all_heads), split_heads(k_own, all_heads), split_heads(v_own, all_heads), pad_bias)
        after_cross = (after_self.astype(jnp.float32) + matmul_f32(context, wo_cross_all)).astype(jnp.bfloat16)

        tokens = batch_dev * dec_len
        experts = w_router.shape[1]
        capacity = (5 * tokens + 4 * experts - 1) // (4 * experts)
        local_experts = experts // ep_size
        assert local_experts == tp_size
        choice = expert_idx.reshape(tokens)
        position = token_positions(choice, experts)
        kept = position < capacity
        owner = choice // local_experts
        owner_row = choice % local_experts
        slots = ep_size * capacity
        slot_here = jnp.where(kept & (owner_row == tp_id), owner * capacity + position, -1)
        pair_slots = 2 * capacity
        code = (owner // 2) * (tp_size * pair_slots) + owner_row * pair_slots + (owner % 2) * capacity + position
        code = jnp.where(kept, code, -1)

        lanes = 128
        w_route = jnp.concatenate([jnp.pad(piece, ((0, 0), (0, lanes - experts))) for piece in split_three(w_router)], axis=1)
        result = expert_exchange(after_cross, slot_here.reshape(batch_dev, 1, dec_len), code[:, None], gain_ffn[None], w_route, w_in, w_out, capacity, experts, ep_size, tp_size)
        return result.reshape(batch_dev, dec_len, d_model)

    return jax.shard_map(layer, mesh=mesh, in_specs=in_specs, out_specs=token_spec, check_vma=False)
```

```python
import functools
import jax
import jax.numpy as jnp
from jax import lax
from jax.experimental import pallas as pl
from jax.experimental.pallas import tpu as pltpu
from jax.sharding import PartitionSpec as P

EPSILON = 1e-6
NEG_LARGE = -1e30


def split_three(weight):
    high = weight.astype(jnp.bfloat16)
    rest = weight - high.astype(jnp.float32)
    mid = rest.astype(jnp.bfloat16)
    low = (rest - mid.astype(jnp.float32)).astype(jnp.bfloat16)
    return high, mid, low


def token_positions(choice, experts):
    tokens = choice.shape[0]
    block = 128
    one_hot = (choice[:, None] == lax.broadcasted_iota(jnp.int32, (tokens, experts), 1)).astype(jnp.bfloat16)
    blocks = one_hot.reshape(tokens // block, block, experts)
    lower = (lax.broadcasted_iota(jnp.int32, (block, block), 0) >= lax.broadcasted_iota(jnp.int32, (block, block), 1)).astype(jnp.bfloat16)
    inside = jnp.einsum('ij,bje->bie', lower, blocks, preferred_element_type=jnp.float32)
    totals = inside[:, -1, :]
    before = jnp.cumsum(totals, axis=0) - totals
    counts = (inside + before[:, None, :]).reshape(tokens, experts)
    return (jnp.sum(counts * one_hot.astype(jnp.float32), axis=-1) - 1.0).astype(jnp.int32)


MESH_ID = pl.DeviceIdType.MESH


def expert_kernel(ep_size, tp_size, capacity, experts, own_ref, slot_ref, code_ref, gain_ref, route_ref, w_in_ref, w_out_ref, out_ref, w_in_buf, w_out_buf, states_buf, gate_buf, send_ref, recv_buf, hidden_buf, out_buf, slot_buf, w_sem, part_send, part_recv, rest_send, rest_recv, disp_send, disp_recv, back_send, back_recv, near_send, near_recv, far_send, far_recv):
    me = lax.axis_index('ep')
    row = lax.axis_index('tp')
    chips = ep_size // 2
    chip = me // 2
    partner = me + 1 - 2 * (me % 2)
    above = (row + 1) % tp_size
    below = (row + tp_size - 1) % tp_size
    across = (row + 2) % tp_size
    own_batch, dec_len, d_model = own_ref.shape
    d_ff = w_in_buf.shape[1]
    pair = 2 * capacity
    tokens = code_ref.shape[0]
    slots = ep_size * capacity
    lanes = 128

    def weight_copies():
        return (pltpu.make_async_copy(w_in_ref.at[row], w_in_buf, w_sem.at[0]),
                pltpu.make_async_copy(w_out_ref.at[row], w_out_buf, w_sem.at[1]))

    copy_in, copy_out = weight_copies()
    copy_in.start()
    copy_out.start()

    barrier = pltpu.get_barrier_semaphore()
    for step in range(1, ep_size):
        pl.semaphore_signal(barrier, inc=1, device_id={'ep': (me + step) % ep_size}, device_id_type=MESH_ID)
    for neighbour in (above, below):
        pl.semaphore_signal(barrier, inc=1, device_id={'tp': neighbour}, device_id_type=MESH_ID)
    pl.semaphore_wait(barrier, ep_size + 1)

    def peers(relative):
        if relative == 0:
            return (partner,)
        first = 2 * ((chip + relative) % chips)
        return (first, first + 1)

    def dispatch_copy(peer, source):
        return pltpu.make_async_remote_copy(
            src_ref=send_ref.at[peer], dst_ref=recv_buf.at[source], send_sem=disp_send.at[peer], recv_sem=disp_recv.at[source],
            device_id={'ep': peer}, device_id_type=MESH_ID)

    def back_copy(peer, source):
        return pltpu.make_async_remote_copy(
            src_ref=out_buf.at[peer], dst_ref=slot_buf.at[row, source], send_sem=back_send.at[peer], recv_sem=back_recv.at[source],
            device_id={'ep': peer}, device_id_type=MESH_ID)

    def near_copy(relative, holder, side, target):
        block = 2 * ((chip + relative) % chips)
        return pltpu.make_async_remote_copy(
            src_ref=slot_buf.at[holder, pl.ds(block, 2)], dst_ref=slot_buf.at[holder, pl.ds(block, 2)],
            send_sem=near_send.at[relative, side], recv_sem=near_recv.at[relative, side],
            device_id={'tp': target}, device_id_type=MESH_ID)

    def far_copy(relative, holder, side, target):
        block = 2 * ((chip + relative) % chips) + side
        return pltpu.make_async_remote_copy(
            src_ref=slot_buf.at[holder, block], dst_ref=slot_buf.at[holder, block],
            send_sem=far_send.at[relative, side], recv_sem=far_recv.at[relative, side],
            device_id={'tp': target}, device_id_type=MESH_ID)

    def part_copy(holder, part, side, target):
        source = own_ref.at[part] if holder is row else states_buf.at[holder, part]
        return pltpu.make_async_remote_copy(
            src_ref=source, dst_ref=states_buf.at[holder, part], send_sem=part_send.at[part, side], recv_sem=part_recv.at[part, side],
            device_id={'tp': target}, device_id_type=MESH_ID)

    def rest_copy(holder, side, target):
        return pltpu.make_async_remote_copy(
            src_ref=states_buf.at[holder, side], dst_ref=states_buf.at[holder, side], send_sem=rest_send.at[side], recv_sem=rest_recv.at[side],
            device_id={'tp': target}, device_id_type=MESH_ID)

    part_copy(row, 0, 0, above).start()
    part_copy(row, 1, 1, below).start()
    part_copy(row, 1, 0, above).start()
    part_copy(row, 0, 1, below).start()
    states_buf[row] = own_ref[...]
    lane_ids = lax.broadcasted_iota(jnp.int32, (1, lanes), 1)
    local = experts // ep_size
    owner = lane_ids // local
    base = (owner // 2) * (tp_size * pair) + (lane_ids % local) * pair + (owner % 2) * capacity

    def absorb(holder, part, fresh):
        block = holder * own_batch + part
        upcast = states_buf[holder, part].astype(jnp.float32)
        mean_sq = jnp.mean(upcast * upcast, axis=-1, keepdims=True)
        normed = (upcast * lax.rsqrt(mean_sq + EPSILON) * gain_ref[...]).astype(jnp.bfloat16)
        wanted = slot_ref[block]
        pick = (wanted == lax.broadcasted_iota(jnp.int32, (slots, dec_len), 0)).astype(jnp.float32).astype(jnp.bfloat16)
        picked = jnp.dot(pick, normed, preferred_element_type=jnp.float32).astype(jnp.bfloat16).reshape(ep_size, capacity, d_model)
        if fresh:
            send_ref[...] = picked
        else:
            send_ref[...] = send_ref[...] + picked
        parts = jnp.dot(normed, route_ref[...], preferred_element_type=jnp.float32)
        logits = parts[:, :lanes] + parts[:, lanes:2 * lanes] + parts[:, 2 * lanes:]
        logits = jnp.where(lane_ids < experts, logits, NEG_LARGE)
        powers = jnp.exp(logits - jnp.max(logits, axis=-1, keepdims=True))
        rows = pl.ds(pl.multiple_of(block * dec_len, dec_len), dec_len)
        place = code_ref[rows, :] - base
        chosen = (place >= 0) & (place < capacity) & (lane_ids < experts)
        gate_buf[rows, :] = jnp.sum(jnp.where(chosen, powers, 0.0), axis=-1, keepdims=True) / jnp.sum(powers, axis=-1, keepdims=True)

    def absorb_pair(first, second):
        def body(step, carry):
            absorb((row + first[0] + step * (second[0] - first[0])) % tp_size, first[1] + step * (second[1] - first[1]), False)
            return carry
        lax.fori_loop(0, 2, body, 0)

    absorb(row, 0, True)
    absorb(row, 1, False)
    part_copy(below, 0, 0, above).wait_recv()
    rest_copy(below, 0, above).start()
    part_copy(above, 1, 1, below).wait_recv()
    rest_copy(above, 1, below).start()
    absorb_pair((tp_size - 1, 0), (tp_size + 1, 1))
    part_copy(below, 1, 0, above).wait_recv()
    part_copy(above, 0, 1, below).wait_recv()
    absorb_pair((tp_size - 1, 1), (tp_size + 1, 0))
    rest_copy(across, 0, above).wait_recv()
    rest_copy(across, 1, below).wait_recv()
    absorb_pair((2, 0), (2, 1))

    compute_order = (0, 1, chips - 1, 2)
    back_order = (0, chips - 1, 1, 2)
    for relative in compute_order:
        for peer in peers(relative):
            dispatch_copy(peer, me).start()
    recv_buf[me] = send_ref[me]

    def compute(relative):
        for peer in peers(relative):
            dispatch_copy(peer, peer).wait_recv()
        if relative == 0:
            copy_in.wait()
        block = 2 * ((chip + relative) % chips)
        inputs = recv_buf[pl.ds(block, 2)].reshape(pair, d_model)
        width = d_ff // 4

        def first(step, carry):
            columns = pl.ds(pl.multiple_of(step * width, width), width)
            hidden = jnp.dot(inputs, w_in_buf[:, columns], preferred_element_type=jnp.float32)
            hidden_buf[:, columns] = jnp.maximum(hidden, 0.0).astype(jnp.bfloat16)
            return carry

        lax.fori_loop(0, 4, first, 0)
        if relative == 0:
            copy_out.wait()
        result = jnp.dot(hidden_buf[...], w_out_buf[...], preferred_element_type=jnp.float32).astype(jnp.bfloat16)
        out_buf[pl.ds(block, 2)] = result.reshape(2, capacity, d_model)
        if relative == 0:
            slot_buf[row, me] = out_buf[me]
        for peer in peers(relative):
            back_copy(peer, me).start()

    def share(relative):
        for peer in peers(relative):
            back_copy(peer, peer).wait_recv()
        near_copy(relative, row, 0, above).start()
        near_copy(relative, row, 1, below).start()

    def forward(relative):
        near_copy(relative, below, 0, above).wait_recv()
        far_copy(relative, below, 0, above).start()
        near_copy(relative, above, 1, below).wait_recv()
        far_copy(relative, above, 1, below).start()

    def combine(relative, fresh):
        far_copy(relative, across, 0, above).wait_recv()
        far_copy(relative, across, 1, below).wait_recv()
        which = (chip + relative) % chips
        values = jnp.concatenate([slot_buf[holder, pl.ds(2 * which, 2)].reshape(pair, d_model) for holder in range(tp_size)], axis=0)
        tile = dec_len

        def body(step, carry):
            previous = states_buf[step // own_batch, step % own_batch] if fresh else out_ref[pl.ds(pl.multiple_of(step * tile, tile), tile), :]
            rows = pl.ds(pl.multiple_of(step * tile, tile), tile)
            wanted = code_ref[rows, :] - which * (tp_size * pair)
            pick = (wanted == lax.broadcasted_iota(jnp.int32, (tile, tp_size * pair), 1)).astype(jnp.float32).astype(jnp.bfloat16)
            picked = jnp.dot(pick, values, preferred_element_type=jnp.float32)
            out_ref[rows, :] = (previous.astype(jnp.float32) + gate_buf[rows, :] * picked).astype(jnp.bfloat16)
            return carry

        lax.fori_loop(0, tokens // tile, body, 0)

    near_1, near_2, near_3 = back_order[1:]
    compute(compute_order[0])
    share(0)
    compute(compute_order[1])
    compute(compute_order[2])
    share(near_1)
    forward(0)
    compute(compute_order[3])
    share(near_2)
    forward(near_1)
    combine(0, True)
    share(near_3)
    forward(near_2)
    combine(near_1, False)
    forward(near_3)
    combine(near_2, False)
    combine(near_3, False)

    for part in (0, 1):
        part_copy(row, part, 0, above).wait_send()
        part_copy(row, part, 1, below).wait_send()
    rest_copy(below, 0, above).wait_send()
    rest_copy(above, 1, below).wait_send()
    for relative in compute_order:
        for peer in peers(relative):
            dispatch_copy(peer, me).wait_send()
            back_copy(peer, me).wait_send()
        near_copy(relative, row, 0, above).wait_send()
        near_copy(relative, row, 1, below).wait_send()
        far_copy(relative, below, 0, above).wait_send()
        far_copy(relative, above, 1, below).wait_send()


def expert_exchange(own, slot_here, code, gain, w_route, w_in, w_out, capacity, experts, ep_size, tp_size):
    d_model = own.shape[2]
    d_ff = w_in.shape[2]
    vmem = pl.BlockSpec(memory_space=pltpu.VMEM)
    anywhere = pl.BlockSpec(memory_space=pl.ANY)
    dma = pltpu.SemaphoreType.DMA
    chips = ep_size // 2
    return pl.pallas_call(
        functools.partial(expert_kernel, ep_size, tp_size, capacity, experts),
        out_shape=jax.ShapeDtypeStruct((code.shape[0], d_model), jnp.bfloat16),
        in_specs=[vmem, vmem, vmem, vmem, vmem, anywhere, anywhere],
        out_specs=vmem,
        scratch_shapes=[
            pltpu.VMEM((d_model, d_ff), jnp.bfloat16),
            pltpu.VMEM((d_ff, d_model), jnp.bfloat16),
            pltpu.VMEM((tp_size,) + own.shape, jnp.bfloat16),
            pltpu.VMEM((code.shape[0], 1), jnp.float32),
            pltpu.VMEM((ep_size, capacity, d_model), jnp.bfloat16),
            pltpu.VMEM((ep_size, capacity, d_model), jnp.bfloat16),
            pltpu.VMEM((2 * capacity, d_ff), jnp.bfloat16),
            pltpu.VMEM((ep_size, capacity, d_model), jnp.bfloat16),
            pltpu.VMEM((tp_size, ep_size, capacity, d_model), jnp.bfloat16),
            dma((2,)), dma((2, 2)), dma((2, 2)), dma((2,)), dma((2,)),
            dma((ep_size,)), dma((ep_size,)), dma((ep_size,)), dma((ep_size,)),
            dma((chips, 2)), dma((chips, 2)), dma((chips, 2)), dma((chips, 2)),
        ],
        compiler_params=pltpu.CompilerParams(collective_id=0, has_side_effects=True),
        name='expert_exchange',
    )(own, slot_here, code, gain, w_route, w_in, w_out)


def attend(queries, key_heads, values, allowed, bias):
    scores = lax.dot_general(queries, key_heads, (((1,), (1,)), ((), ())), preferred_element_type=jnp.float32)
    if bias is not None:
        scores = scores + bias
    scores = jnp.where(allowed, scores, NEG_LARGE)
    powers = jnp.exp(scores - jnp.max(scores, axis=-1, keepdims=True))
    weights = (powers / jnp.sum(powers, axis=-1, keepdims=True)).astype(jnp.bfloat16)
    return jnp.dot(weights, values, preferred_element_type=jnp.float32).astype(jnp.bfloat16)


def attention_kernel(tp_size, heads, dec_ref, enc_ref, pad_ref, bias_ref, gain_self_ref, gain_cross_ref, wq_ref, wk_ref, wv_ref, wo_ref, wq_cross_ref, wk_cross_ref, wv_cross_ref, wo_cross_ref, out_ref, dec_buf, enc_buf, weight_buf, kv_send, kv_recv, kv_relay, ctx_send, ctx_recv, ctx_relay, mixed_buf, dec_sem, enc_sem, wn_send, wn_recv, wf_send, wf_recv, wp_send, wp_recv, kv_sems, ctx_sems):
    me = lax.axis_index('ep')
    row = lax.axis_index('tp')
    core = me % 2
    partner = me + 1 - 2 * core
    above = (row + 1) % tp_size
    below = (row + tp_size - 1) % tp_size
    across = (row + 2) % tp_size
    width = wo_ref.shape[0]
    head = width // heads
    batch_dev, dec_len, d_model = dec_ref.shape
    enc_len = enc_ref.shape[1]

    enc_copy = pltpu.make_async_copy(enc_ref, enc_buf, enc_sem.at[0])
    enc_copy.start()

    def dec_copy(block):
        return pltpu.make_async_copy(dec_ref.at[pl.ds(2 * block, 2)], dec_buf.at[pl.ds(2 * block, 2)], dec_sem.at[block])

    for block in range(tp_size):
        dec_copy(block).start()

    barrier = pltpu.get_barrier_semaphore()
    pl.semaphore_signal(barrier, inc=1, device_id={'ep': partner}, device_id_type=MESH_ID)
    for neighbour in (above, below):
        pl.semaphore_signal(barrier, inc=1, device_id={'tp': neighbour}, device_id_type=MESH_ID)

    weight_buf[row, 0:width] = wo_ref[...]
    weight_buf[row, width:2 * width] = wq_cross_ref[...].astype(jnp.float32).T.astype(jnp.bfloat16)
    weight_buf[row, 2 * width:3 * width] = wo_cross_ref[...]
    pl.semaphore_wait(barrier, 3)

    groups = ((0, 2 * width), (2 * width, width))

    def near_weights(group, holder, side, target):
        start, size = groups[group]
        rows = pl.ds(pl.multiple_of(start + core * (size // 2), 32), size // 2)
        return pltpu.make_async_remote_copy(
            src_ref=weight_buf.at[holder, rows], dst_ref=weight_buf.at[holder, rows],
            send_sem=wn_send.at[group, side], recv_sem=wn_recv.at[group, side],
            device_id={'tp': target}, device_id_type=MESH_ID)

    def far_weights(group, holder, side, target):
        start, size = groups[group]
        rows = pl.ds(pl.multiple_of(start + core * (size // 2) + side * (size // 4), 16), size // 4)
        return pltpu.make_async_remote_copy(
            src_ref=weight_buf.at[holder, rows], dst_ref=weight_buf.at[holder, rows],
            send_sem=wf_send.at[group, side], recv_sem=wf_recv.at[group, side],
            device_id={'tp': target}, device_id_type=MESH_ID)

    def pass_weights(group, holder, which, half):
        start, size = groups[group]
        rows = pl.ds(pl.multiple_of(start + half * (size // 2), 32), size // 2)
        return pltpu.make_async_remote_copy(
            src_ref=weight_buf.at[holder, rows], dst_ref=weight_buf.at[holder, rows],
            send_sem=wp_send.at[group, which], recv_sem=wp_recv.at[group, which],
            device_id={'ep': partner}, device_id_type=MESH_ID)

    def exchange(sent, received, relay, sems):
        half = dec_len // 2

        def near(block, source, side, target):
            return pltpu.make_async_remote_copy(
                src_ref=sent.at[block], dst_ref=received.at[source], send_sem=sems.at[0, side], recv_sem=sems.at[1, side],
                device_id={'tp': target}, device_id_type=MESH_ID)

        def first_hop(side, target):
            return pltpu.make_async_remote_copy(
                src_ref=sent.at[across, pl.ds(side * half, half)], dst_ref=relay.at[side], send_sem=sems.at[2, side], recv_sem=sems.at[3, side],
                device_id={'tp': target}, device_id_type=MESH_ID)

        def second_hop(source, side, target):
            return pltpu.make_async_remote_copy(
                src_ref=relay.at[side], dst_ref=received.at[source, pl.ds(side * half, half)], send_sem=sems.at[4, side], recv_sem=sems.at[5, side],
                device_id={'tp': target}, device_id_type=MESH_ID)

        def start():
            first_hop(0, above).start()
            first_hop(1, below).start()
            near(above, row, 0, above).start()
            near(below, row, 1, below).start()

        def relay_on():
            first_hop(0, above).wait_recv()
            second_hop(below, 0, above).start()
            first_hop(1, below).wait_recv()
            second_hop(above, 1, below).start()

        def finish():
            near(above, below, 0, above).wait_recv()
            near(below, above, 1, below).wait_recv()
            second_hop(across, 0, above).wait_recv()
            second_hop(across, 1, below).wait_recv()

        def drain():
            first_hop(0, above).wait_send()
            first_hop(1, below).wait_send()
            near(above, row, 0, above).wait_send()
            near(below, row, 1, below).wait_send()
            second_hop(below, 0, above).wait_send()
            second_hop(above, 1, below).wait_send()

        return start, relay_on, finish, drain

    kv_start, kv_relay_on, kv_finish, kv_drain = exchange(kv_send, kv_recv, kv_relay, kv_sems)
    ctx_start, ctx_relay_on, ctx_finish, ctx_drain = exchange(ctx_send, ctx_recv, ctx_relay, ctx_sems)

    near_weights(0, row, 0, above).start()
    near_weights(0, row, 1, below).start()

    enc_copy.wait()

    def project_kv(block, carry):
        source = enc_buf[pl.ds(2 * block, 2)].reshape(2 * enc_len, d_model)
        keys = jnp.dot(source, wk_cross_ref[...], preferred_element_type=jnp.float32).astype(jnp.bfloat16)
        values = jnp.dot(source, wv_cross_ref[...], preferred_element_type=jnp.float32).astype(jnp.bfloat16)
        kv_send[block] = jnp.concatenate([keys, values], axis=-1)
        return carry

    lax.fori_loop(0, tp_size, project_kv, 0)
    kv_start()

    causal = lax.broadcasted_iota(jnp.int32, (dec_len, dec_len), 1) <= lax.broadcasted_iota(jnp.int32, (dec_len, dec_len), 0)

    def normalise(upcast, gain):
        mean_sq = jnp.mean(upcast * upcast, axis=-1, keepdims=True)
        return (upcast * lax.rsqrt(mean_sq + EPSILON) * gain).astype(jnp.bfloat16)

    def self_block(block, carry):
        dec_copy(block).wait()
        normed = normalise(dec_buf[pl.ds(2 * block, 2)].reshape(2 * dec_len, d_model).astype(jnp.float32), gain_self_ref[...])
        queries = jnp.dot(normed, wq_ref[...], preferred_element_type=jnp.float32).astype(jnp.bfloat16)
        keys = jnp.dot(normed, wk_ref[...], preferred_element_type=jnp.float32).astype(jnp.bfloat16)
        values = jnp.dot(normed, wv_ref[...], preferred_element_type=jnp.float32).astype(jnp.bfloat16)
        pieces = []
        for seq in range(2):
            rows = slice(seq * dec_len, (seq + 1) * dec_len)
            for which in range(heads):
                lanes = slice(which * head, (which + 1) * head)
                pieces.append(attend(queries[rows, lanes], keys[rows, lanes], values[rows, lanes], causal, bias_ref[which]))
        ctx_send[block] = jnp.concatenate(pieces, axis=-1)
        return carry

    lax.fori_loop(0, tp_size, self_block, 0)
    ctx_start()
    ctx_recv[row] = ctx_send[row]
    kv_recv[row] = kv_send[row]

    def weights_forward(group):
        near_weights(group, below, 0, above).wait_recv()
        far_weights(group, below, 0, above).start()
        pass_weights(group, below, 0, core).start()
        near_weights(group, above, 1, below).wait_recv()
        far_weights(group, above, 1, below).start()
        pass_weights(group, above, 1, core).start()

    def weights_pass_far(group):
        far_weights(group, across, 0, above).wait_recv()
        far_weights(group, across, 1, below).wait_recv()
        pass_weights(group, across, 2, core).start()

    def weights_finish(group):
        pass_weights(group, below, 0, 1 - core).wait_recv()
        pass_weights(group, above, 1, 1 - core).wait_recv()
        pass_weights(group, across, 2, 1 - core).wait_recv()

    weights_forward(0)
    kv_relay_on()
    near_weights(1, row, 0, above).start()
    near_weights(1, row, 1, below).start()
    weights_pass_far(0)
    weights_finish(0)
    ctx_relay_on()
    ctx_finish()

    for seq in range(2):
        update = None
        for source in range(tp_size):
            context = ctx_recv[source, :, seq * width:(seq + 1) * width]
            term = jnp.dot(context, weight_buf[source, 0:width], preferred_element_type=jnp.float32)
            update = term if update is None else update + term
        out_ref[seq] = (dec_buf[2 * row + seq].astype(jnp.float32) + update).astype(jnp.bfloat16)
    weights_forward(1)
    kv_finish()
    normed = normalise(out_ref[...].reshape(2 * dec_len, d_model).astype(jnp.float32), gain_cross_ref[...])

    def cross_block(source, carry):
        queries = lax.dot_general(normed, weight_buf[source, width:2 * width], (((1,), (1,)), ((), ())), preferred_element_type=jnp.float32).astype(jnp.bfloat16)
        key_values = kv_recv[source]
        for seq in range(2):
            allowed = pad_ref[pl.ds(2 * row + seq, 1), :] == 0
            rows = slice(seq * dec_len, (seq + 1) * dec_len)
            key_rows = slice(seq * enc_len, (seq + 1) * enc_len)
            pieces = []
            for which in range(heads):
                lanes = slice(which * head, (which + 1) * head)
                value_lanes = slice(width + which * head, width + (which + 1) * head)
                pieces.append(attend(queries[rows, lanes], key_values[key_rows, lanes], key_values[key_rows, value_lanes], allowed, None))
            mixed_buf[source, rows] = jnp.concatenate(pieces, axis=-1)
        return carry

    lax.fori_loop(0, tp_size, cross_block, 0)
    weights_pass_far(1)
    weights_finish(1)
    for seq in range(2):
        update = None
        for source in range(tp_size):
            context = mixed_buf[source, seq * dec_len:(seq + 1) * dec_len]
            term = jnp.dot(context, weight_buf[source, 2 * width:3 * width], preferred_element_type=jnp.float32)
            update = term if update is None else update + term
        out_ref[seq] = (out_ref[seq].astype(jnp.float32) + update).astype(jnp.bfloat16)

    kv_drain()
    ctx_drain()
    for group in range(2):
        near_weights(group, row, 0, above).wait_send()
        near_weights(group, row, 1, below).wait_send()
        far_weights(group, below, 0, above).wait_send()
        far_weights(group, above, 1, below).wait_send()
        pass_weights(group, below, 0, core).wait_send()
        pass_weights(group, above, 1, core).wait_send()
        pass_weights(group, across, 2, core).wait_send()


def attention_front(arrays, heads, tp_size):
    dec_states, enc_states, wo_self = arrays[0], arrays[1], arrays[9]
    batch_dev, dec_len, d_model = dec_states.shape
    enc_len = enc_states.shape[1]
    width = wo_self.shape[0]
    vmem = pl.BlockSpec(memory_space=pltpu.VMEM)
    anywhere = pl.BlockSpec(memory_space=pl.ANY)
    dma = pltpu.SemaphoreType.DMA
    block = (tp_size, dec_len, 2 * width)
    relay = (2, dec_len // 2, 2 * width)
    return pl.pallas_call(
        functools.partial(attention_kernel, tp_size, heads),
        out_shape=jax.ShapeDtypeStruct((batch_dev // tp_size, dec_len, d_model), jnp.bfloat16),
        in_specs=[anywhere, anywhere] + [vmem] * (len(arrays) - 2),
        out_specs=vmem,
        scratch_shapes=[
            pltpu.VMEM(dec_states.shape, jnp.bfloat16),
            pltpu.VMEM(enc_states.shape, jnp.bfloat16),
            pltpu.VMEM((tp_size, 3 * width, d_model), jnp.bfloat16),
            pltpu.VMEM(block, jnp.bfloat16), pltpu.VMEM(block, jnp.bfloat16), pltpu.VMEM(relay, jnp.bfloat16),
            pltpu.VMEM(block, jnp.bfloat16), pltpu.VMEM(block, jnp.bfloat16), pltpu.VMEM(relay, jnp.bfloat16),
            pltpu.VMEM((tp_size, 2 * dec_len, width), jnp.bfloat16),
            dma((tp_size,)), dma((1,)),
            dma((2, 2)), dma((2, 2)), dma((2, 2)), dma((2, 2)), dma((2, 3)), dma((2, 3)),
            dma((6, 2)), dma((6, 2)),
        ],
        compiler_params=pltpu.CompilerParams(collective_id=1, has_side_effects=True),
        name='attention_front',
    )(*arrays)


def solution(mesh):
    ep_size = mesh.shape['ep']
    tp_size = mesh.shape['tp']
    token_spec = P(('part', 'ep'), None, None)
    row_spec = P(('part', 'ep'), None)
    col_spec = P(None, 'tp')
    head_rows = P('tp', None)
    vec_spec = P(None)
    expert_spec = P('ep', None, None)
    in_specs = (token_spec, token_spec, row_spec, row_spec, P('tp', None, None), vec_spec, col_spec, col_spec, col_spec, head_rows, vec_spec, col_spec, col_spec, col_spec, head_rows, vec_spec, P(None, None), expert_spec, expert_spec)

    def layer(dec_states, enc_states, enc_pad, expert_idx, self_bias, gain_self, wq_self, wk_self, wv_self, wo_self, gain_cross, wq_cross, wk_cross, wv_cross, wo_cross, gain_ffn, w_router, w_in, w_out):
        batch_dev, dec_len, d_model = dec_states.shape
        heads = self_bias.shape[0]
        tp_id = lax.axis_index('tp')
        after_cross = attention_front([dec_states, enc_states, enc_pad, self_bias, gain_self[None], gain_cross[None], wq_self, wk_self, wv_self, wo_self, wq_cross, wk_cross, wv_cross, wo_cross], heads, tp_size)

        tokens = batch_dev * dec_len
        experts = w_router.shape[1]
        capacity = (5 * tokens + 4 * experts - 1) // (4 * experts)
        local_experts = experts // ep_size
        assert local_experts == tp_size
        choice = expert_idx.reshape(tokens)
        position = token_positions(choice, experts)
        kept = position < capacity
        owner = choice // local_experts
        owner_row = choice % local_experts
        slots = ep_size * capacity
        slot_here = jnp.where(kept & (owner_row == tp_id), owner * capacity + position, -1)
        pair_slots = 2 * capacity
        code = (owner // 2) * (tp_size * pair_slots) + owner_row * pair_slots + (owner % 2) * capacity + position
        code = jnp.where(kept, code, -1)

        lanes = 128
        w_route = jnp.concatenate([jnp.pad(piece, ((0, 0), (0, lanes - experts))) for piece in split_three(w_router)], axis=1)
        result = expert_exchange(after_cross, slot_here.reshape(batch_dev, 1, dec_len), code[:, None], gain_ffn[None], w_route, w_in, w_out, capacity, experts, ep_size, tp_size)
        return result.reshape(batch_dev, dec_len, d_model)

    return jax.shard_map(layer, mesh=mesh, in_specs=in_specs, out_specs=token_spec, check_vma=False)
```
